32 devices in a mesh: tm: 16 (over z, y, core), space: 2 (over x).
Axes of the slice: x: 2, y: 2, z: 4, core: 2. Of those that a mesh axis runs over, the one named last changes fastest.
Arguments:
- control: float32 [32, 512], P('space'), may hold values from -0.6 to 0.6
- initial: float32 [32, 512], P('space'), may hold values from -6 to 6
- diffusion: float32 [32, 512], P('space'), may hold values from 0.1 to 1
- reaction: float32 [32, 512], P('space'), may hold values from 7.8125e-05 to 0.1
- forward_guess: float32 [16, 32, 512], P('tm', 'space'), may hold values from -1.5 to 1.5
- adjoint_guess: float32 [16, 32, 512], P('tm', 'space'), may hold values from -1.5 to 1.5
- observed: float32 [16, 32, 512], P('tm', 'space'), may hold values from -6 to 6
Outputs:
- forward_states: float32 [16, 32, 512], P('tm', 'space')
- adjoint_states: float32 [16, 32, 512], P('tm', 'space')
- control_gradient: float32 [32, 512], P('space')
The draws below stay inside these ranges and needn't reach their ends.
All inputs are finite; a program needn't handle non-finite values.
Results may differ from the reference program's by a relative error of at most 0.00015.
Values sent between devices are 32-bit elements; how exact they have to be, the bound alone decides.
A program may use at most 128 MiB of HBM per device.

```python
import math
import jax
import jax.numpy as jnp
from jax import lax

COLS = 512
SWEEPS = 3
COARSEN = 8
SLABS = 16
NX = 32
STEPS = 128


def shard_levels(key, extent, pieces, low, top_value):
    loudness, own = 1.0, jax.random.fold_in(key, 6)
    for axis_at, parts in pieces:
        heights = jnp.exp(jax.random.uniform(jax.random.fold_in(own, axis_at), (parts,), jnp.float32, low / len(pieces), top_value / len(pieces)))
        loudness = loudness * jnp.repeat(heights, extent[axis_at] // parts).reshape([-1 if axis == axis_at else 1 for axis in range(len(extent))])
    return loudness


def gaussian(stream_key, extent, width, bound, pieces=(), dtype=jnp.bfloat16):
    level = shard_levels(stream_key, extent, pieces, -0.22, 0.18) if pieces else 1.0
    array = jax.random.normal(stream_key, extent, jnp.float32) * width * level
    return jnp.minimum(jnp.maximum(array, -bound), bound).astype(dtype)


def setup_inputs(seed: int = 0) -> dict:
    streams_of = jax.random.split(jax.random.key(seed), 8)
    control = gaussian(streams_of[0], (NX, COLS), 0.1, 0.6, ((0, 2),), jnp.float32)
    initial = gaussian(streams_of[1], (NX, COLS), 1.0, 6.0, ((0, 2),), jnp.float32)
    diffusion = jnp.clip(jnp.exp(math.log(1.0) - 2.3025851 * jax.random.uniform(streams_of[2], (NX, COLS), jnp.float32) ** shard_levels(streams_of[2], (NX, COLS), ((0, 2),), -0.2, 0.2)), 0.1, 1.0)
    reaction = jnp.clip(jnp.exp(math.log(0.1) - 7.1546154 * jax.random.uniform(streams_of[3], (NX, COLS), jnp.float32) ** shard_levels(streams_of[3], (NX, COLS), ((0, 2),), -0.2, 0.2)), 7.812499825377017e-05, 0.1)
    forward_guess = gaussian(streams_of[4], (SLABS, NX, COLS), 0.25, 1.5, ((0, 16), (1, 2)), jnp.float32)
    adjoint_guess = gaussian(streams_of[5], (SLABS, NX, COLS), 0.25, 1.5, ((0, 16), (1, 2)), jnp.float32)
    observed = gaussian(streams_of[6], (SLABS, NX, COLS), 1.0, 6.0, ((0, 16), (1, 2)), jnp.float32)
    return dict(control=control, initial=initial, diffusion=diffusion, reaction=reaction, forward_guess=forward_guess, adjoint_guess=adjoint_guess, observed=observed)


def neighbours(source):
    zero_row = jnp.zeros_like(source[..., :1, :])
    zero_column = jnp.zeros_like(source[..., :, :1])
    vertical = jnp.concatenate([source[..., 1:, :], zero_row], -2) + jnp.concatenate([zero_row, source[..., :-1, :]], -2)
    lateral = jnp.concatenate([source[..., :, 1:], zero_column], -1) + jnp.concatenate([zero_column, source[..., :, :-1]], -1)
    return vertical + lateral


def reference(control, initial, diffusion, reaction, forward_guess, adjoint_guess, observed):
    diagonal = 1.0 + 4.0 * diffusion + reaction
    weight = diffusion / diagonal

    def forward_map(rhs_field):
        iterate = rhs_field
        for number in range(SWEEPS):
            iterate = (rhs_field + diffusion * neighbours(iterate)) / diagonal
        return iterate

    def adjoint_map(rhs_field):
        carried = rhs_field
        summed = rhs_field
        for number in range(SWEEPS - 1):
            carried = neighbours(weight * carried)
            summed = summed + carried
        return summed / diagonal + neighbours(weight * carried)

    zero_slab = jnp.zeros_like(forward_guess[:1])

    def relax(own_forward, own_adjoint, first_pass):
        current = jnp.concatenate([initial[None], own_forward[:-1]], 0)
        states = []
        for number in range(COARSEN - 1):
            current = forward_map(current + control)
            states.append(current)
        points = states + [own_forward]
        current = jnp.concatenate([own_adjoint[1:], zero_slab], 0)
        fine_total = jnp.zeros_like(own_adjoint)
        for position in range(COARSEN, 1, -1):
            current = adjoint_map(current + (points[position - 1] - observed) / COARSEN)
            fine_total = fine_total + current
        if first_pass:
            forward_residual = forward_map(states[-1] + control) - own_forward
            adjoint_residual = adjoint_map(current + (points[0] - observed) / COARSEN) - own_adjoint
            return forward_residual, adjoint_residual
        return fine_total

    forward_residual, adjoint_residual = relax(forward_guess, adjoint_guess, True)
    damping = 1.0 / (1.0 + COARSEN * reaction)

    def coarse_chain(running, increment):
        running = damping * running + increment
        return running, running

    zero_field = jnp.zeros_like(initial)
    forward_correction = lax.scan(coarse_chain, zero_field, forward_residual)[1]
    adjoint_correction = lax.scan(coarse_chain, zero_field, adjoint_residual, reverse=True)[1]
    forward_states = forward_guess + forward_correction
    adjoint_states = adjoint_guess + adjoint_correction
    fine_total = relax(forward_states, adjoint_states, False)
    control_gradient = (jnp.sum(adjoint_states, 0) + jnp.sum(fine_total, 0)) / STEPS
    return forward_states, adjoint_states, control_gradient
```

```python
import functools

import jax
import jax.numpy as jnp
from jax import lax
from jax.experimental import pallas as pl
from jax.experimental.pallas import tpu as pltpu
from jax.sharding import PartitionSpec as P

SWEEPS = 3
COARSEN = 8
SUB, LANES = 8, 128
MESH = pl.DeviceIdType.MESH

CONTROL, DIFFUSION, REACTION, ENTRY, GUESS, TARGET, FORWARD, EXIT, INITIAL, ADJOINT = range(10)
SLOTS = 10
SUM_ENTRY, SUM_STATES, SUM_TARGET, SUM_EXIT, SUM_ADJOINT = range(5)


def kernel(
    T, X,
    control_ref, initial_ref, diffusion_ref, reaction_ref, guess_ref, adjoint_ref, observed_ref,
    states_out, adjoints_out, gradient_out,
    full, weight, inverse, points, total, sums, gathered, gathered_adj, solved, solved_adj,
    packed, packed_adj, landed, landed_adj,
    in_send, in_recv, m1_send, m1_recv, m2_send, m2_recv,
    b1_send, b1_recv, b2_send, b2_recv, p1_send, p1_recv, p2_send, p2_recv,
):
    rows, cols = control_ref.shape
    grid_rows = rows * X
    col_tiles = cols // LANES
    tiles = (grid_rows // SUB) * col_tiles
    own_tiles = (rows // SUB) * col_tiles
    stride = T // tiles
    j = lax.axis_index("tm")
    x = lax.axis_index("space")
    first, last = j == 0, j == T - 1

    def device(tm, space):
        return {"tm": tm, "space": space}

    def side(o):
        return lax.rem(x + o, X)

    def from_side(o):
        return lax.rem(x + X - o, X)

    barrier = pltpu.get_barrier_semaphore()

    def greet(tm, space):
        pl.semaphore_signal(barrier, inc=1, device_id=device(tm, space), device_id_type=MESH)

    def greet_plane(i, c):
        greet(lax.rem(j + i, T), x)
        return c

    for o in range(1, X):
        greet(j, side(o))

        @pl.when(j > 0)
        def _():
            greet(j - 1, side(o))

        @pl.when(j < T - 1)
        def _():
            greet(j + 1, side(o))

    lax.fori_loop(1, T, greet_plane, 0)

    def block_rows(space):
        return pl.ds(pl.multiple_of(space * rows, rows), rows)

    own = block_rows(x)
    full[CONTROL, own, :] = control_ref[...]
    full[DIFFUSION, own, :] = diffusion_ref[...]
    full[REACTION, own, :] = reaction_ref[...]
    full[GUESS, own, :] = guess_ref[0]
    full[TARGET, own, :] = observed_ref[0]
    full[INITIAL, own, :] = initial_ref[...]

    @pl.when(first)
    def _():
        full[ENTRY, own, :] = initial_ref[...]

    @pl.when(last)
    def _():
        full[EXIT] = jnp.zeros((grid_rows, cols), jnp.float32)

    neighbours_count = (j > 0).astype(jnp.int32) + (j < T - 1).astype(jnp.int32)
    pl.semaphore_wait(barrier, (T - 1) + (X - 1) * (1 + neighbours_count))

    def send(src, slot, o, tm):
        return pltpu.make_async_remote_copy(
            src_ref=src, dst_ref=full.at[slot, own, :],
            send_sem=in_send.at[slot, o], recv_sem=in_recv.at[slot, o],
            device_id=device(tm, side(o)), device_id_type=MESH,
        )

    def entry_copy(o):
        return send(guess_ref.at[0], ENTRY, o, j + 1)

    def initial_entry_copy(o):
        return pltpu.make_async_remote_copy(
            src_ref=initial_ref, dst_ref=full.at[ENTRY, own, :],
            send_sem=in_send.at[FORWARD, o], recv_sem=in_recv.at[ENTRY, o],
            device_id=device(j, side(o)), device_id_type=MESH,
        )

    def exit_copy(o):
        return send(adjoint_ref.at[0], EXIT, o, j - 1)

    def input_sends(act):
        for o in range(1, X):
            act(send(diffusion_ref, DIFFUSION, o, j))
            act(send(reaction_ref, REACTION, o, j))
            act(send(control_ref, CONTROL, o, j))

            @pl.when(first)
            def _():
                act(initial_entry_copy(o))

        @pl.when(j < T - 1)
        def _():
            for o in range(X):
                act(entry_copy(o))

        for o in range(1, X):
            act(send(guess_ref.at[0], GUESS, o, j))
            act(send(observed_ref.at[0], TARGET, o, j))

        @pl.when(j > 0)
        def _():
            for o in range(X):
                act(exit_copy(o))

        for o in range(1, X):
            act(send(initial_ref, INITIAL, o, j))

    def await_input(slot, o):
        pltpu.make_async_remote_copy(
            src_ref=control_ref, dst_ref=full.at[slot, block_rows(from_side(o)), :],
            send_sem=in_send.at[slot, o], recv_sem=in_recv.at[slot, o],
            device_id=device(j, side(o)), device_id_type=MESH,
        ).wait_recv()

    input_sends(lambda copy: copy.start())

    lane = lax.broadcasted_iota(jnp.int32, (grid_rows, LANES), 1)
    row = lax.broadcasted_iota(jnp.int32, (grid_rows, LANES), 0)
    lane_low, lane_high = lane == 0, lane == LANES - 1
    row_low, row_high = row == 0, row == grid_rows - 1
    blocks = range(col_tiles)
    zero = jnp.zeros((grid_rows, LANES), jnp.float32)

    def cut(value):
        return [value[:, b * LANES : (b + 1) * LANES] for b in blocks]

    def get(ref, *index):
        return [ref[(*index, slice(None), pl.ds(b * LANES, LANES))] for b in blocks]

    def put(ref, value, *index):
        for b in blocks:
            ref[(*index, slice(None), pl.ds(b * LANES, LANES))] = value[b]

    def zipped(f, *lists):
        return [f(*items) for items in zip(*lists)]

    def neighbours(v):
        right = [pltpu.roll(b, LANES - 1, 1) for b in v]
        left = [pltpu.roll(b, 1, 1) for b in v]
        out = []
        for b in blocks:
            up = jnp.where(row_low, 0.0, pltpu.roll(v[b], 1, 0))
            down = jnp.where(row_high, 0.0, pltpu.roll(v[b], grid_rows - 1, 0))
            to_right = jnp.where(lane_high, right[b + 1] if b + 1 < col_tiles else zero, right[b])
            to_left = jnp.where(lane_low, left[b - 1] if b > 0 else zero, left[b])
            out.append((up + down) + (to_right + to_left))
        return out

    def forward_step(v, scale):
        rhs = zipped(lambda a, c: a + scale * c, v, get(full, CONTROL))
        w = get(weight)
        base = zipped(lambda a, c: a * c, rhs, get(inverse))
        iterate = rhs
        for _ in range(SWEEPS):
            iterate = zipped(lambda a, c, n: a + c * n, base, w, neighbours(iterate))
        return iterate

    def adjoint_step(y):
        w = get(weight)
        carried, summed = y, y
        for _ in range(SWEEPS - 1):
            carried = neighbours(zipped(lambda a, c: a * c, w, carried))
            summed = zipped(lambda a, c: a + c, summed, carried)
        tail = neighbours(zipped(lambda a, c: a * c, w, carried))
        return zipped(lambda a, c, t: a * c + t, summed, get(inverse), tail)

    def misfit_added(g, point, target):
        return zipped(lambda a, p, o: a + (p - o) * (1.0 / COARSEN), g, point, target)

    for o in range(1, X):
        await_input(DIFFUSION, o)
        await_input(REACTION, o)
    spread = full[DIFFUSION]
    diagonal = 1.0 + 4.0 * spread + full[REACTION]
    reciprocal = 1.0 / diagonal
    inverse[...] = reciprocal
    weight[...] = spread * reciprocal

    def forward_points(start, scale):
        def body(i, v):
            v = forward_step(v, scale)
            put(points, v, i)
            return v

        return lax.fori_loop(0, COARSEN - 1, body, start)

    for o in range(1, X):
        await_input(CONTROL, o)
        await_input(ENTRY, o)

    @pl.when(j > 0)
    def _():
        await_input(ENTRY, 0)

    damping = 1.0 / (1.0 + COARSEN * full[REACTION])

    v = forward_points(get(full, ENTRY), 1.0)
    v = forward_step(v, 1.0)
    keep = (j > 0).astype(jnp.float32)
    put(full, zipped(lambda a, d, s: a - keep * (d * s), v, cut(damping), get(full, ENTRY)), FORWARD)

    for o in range(1, X):
        await_input(GUESS, o)
        await_input(TARGET, o)
        await_input(INITIAL, o)

    def tile_rows(d):
        return pl.ds(pl.multiple_of((d // col_tiles) * SUB, SUB), SUB)

    def tile_cols(d):
        return pl.ds(pl.multiple_of(lax.rem(d, col_tiles) * LANES, LANES), LANES)

    mine = j // stride
    owner = jnp.logical_and(lax.rem(j, stride) == 0, mine < tiles)
    my_rows, my_cols = tile_rows(lax.rem(mine, tiles)), tile_cols(lax.rem(mine, tiles))

    def scatter(act, source, target, send_sem, recv_sem):
        def body(i, c):
            d = lax.rem(mine + i, tiles)

            @pl.when(d * stride != j)
            def _():
                act(pltpu.make_async_remote_copy(
                    src_ref=source(tile_rows(d), tile_cols(d)), dst_ref=target.at[j],
                    send_sem=send_sem.at[d], recv_sem=recv_sem.at[j],
                    device_id=device(d * stride, x), device_id_type=MESH,
                ))

            return c

        lax.fori_loop(0, tiles, body, 0)

    def source_forward(r, c):
        return full.at[pl.ds(TARGET, 2), r, c]

    def source_adjoint(r, c):
        return full.at[ADJOINT, r, c]

    def await_gather(source, target, send_sem, recv_sem):
        def body(i, c):
            k = lax.rem(j + i, T)
            pltpu.make_async_remote_copy(
                src_ref=source(my_rows, my_cols), dst_ref=target.at[k],
                send_sem=send_sem.at[0], recv_sem=recv_sem.at[k],
                device_id=device(k, x), device_id_type=MESH,
            ).wait_recv()
            return c

        lax.fori_loop(1, T, body, 0)

    def spread_sums(act, source, slot, count, send_sem, recv_sem):
        def body(i, c):
            k = lax.rem(j + i, T)
            act(pltpu.make_async_remote_copy(
                src_ref=source, dst_ref=sums.at[pl.ds(slot, count), my_rows, my_cols],
                send_sem=send_sem.at[k], recv_sem=recv_sem.at[mine],
                device_id=device(k, x), device_id_type=MESH,
            ))
            return c

        lax.fori_loop(1, T, body, 0)

    def await_sums(source, slot, count, send_sem, recv_sem):
        def body(d, c):
            @pl.when(d * stride != j)
            def _():
                pltpu.make_async_remote_copy(
                    src_ref=source, dst_ref=sums.at[pl.ds(slot, count), tile_rows(d), tile_cols(d)],
                    send_sem=send_sem.at[0], recv_sem=recv_sem.at[d],
                    device_id=device(d * stride, x), device_id_type=MESH,
                ).wait_recv()

            return c

        lax.fori_loop(0, tiles, body, 0)

    local = mine - x * own_tiles
    holds_output = jnp.logical_and(owner, jnp.logical_and(local >= 0, local < own_tiles))
    local_tile = lax.rem(local + tiles, own_tiles)

    def spread_solved(act, source, target, send_sem, recv_sem):
        def body(i, c):
            k = lax.rem(j + i, T)
            act(pltpu.make_async_remote_copy(
                src_ref=source.at[k], dst_ref=target.at[tile_rows(local_tile), tile_cols(local_tile)],
                send_sem=send_sem.at[k], recv_sem=recv_sem.at[local_tile],
                device_id=device(k, x), device_id_type=MESH,
            ))
            return c

        lax.fori_loop(1, T, body, 0)

    def await_solved(source, target, send_sem, recv_sem):
        def body(d, c):
            source_tm = (d + x * own_tiles) * stride

            @pl.when(source_tm != j)
            def _():
                pltpu.make_async_remote_copy(
                    src_ref=source.at[0], dst_ref=target.at[tile_rows(d), tile_cols(d)],
                    send_sem=send_sem.at[0], recv_sem=recv_sem.at[d],
                    device_id=device(source_tm, x), device_id_type=MESH,
                ).wait_recv()

            return c

        lax.fori_loop(0, own_tiles, body, 0)

    start = lambda copy: copy.start()
    finish = lambda copy: copy.wait_send()

    scatter(start, source_forward, gathered, m1_send, m1_recv)

    @pl.when(j < T - 1)
    def _():
        for o in range(X):
            await_input(EXIT, o)

    def adjoint_points(g, target):
        def body(i, g):
            at = COARSEN - 2 - i
            return adjoint_step(misfit_added(g, get(points, at), get(*target)))

        return body

    g = adjoint_step(misfit_added(get(full, EXIT), get(full, GUESS), get(full, TARGET)))
    g = lax.fori_loop(0, COARSEN - 1, adjoint_points(g, (full, TARGET)), g)
    put(full, zipped(lambda a, d, t: a - d * t, g, cut(damping), get(full, EXIT)), ADJOINT)
    scatter(start, source_adjoint, gathered_adj, m2_send, m2_recv)

    @pl.when(owner)
    def _():
        my_damping = 1.0 / (1.0 + COARSEN * full[REACTION, my_rows, my_cols])
        gathered[j] = full[pl.ds(TARGET, 2), my_rows, my_cols]
        await_gather(source_forward, gathered, m1_send, m1_recv)

        def body(k, carry):
            state, before, through, target = carry
            state = my_damping * state + gathered[k, 1]
            solved[k] = state
            return (state, through, through + state, target + gathered[k, 0])

        head = gathered[0, 1]
        solved[0] = head
        _, before, through, target = lax.fori_loop(1, T, body, (head, head, head, gathered[0, 0]))
        for slot, value in ((SUM_ENTRY, before), (SUM_STATES, through), (SUM_TARGET, target)):
            packed[slot] = value
            sums[slot, my_rows, my_cols] = value
        spread_sums(start, packed, SUM_ENTRY, 3, b1_send, b1_recv)

    @pl.when(holds_output)
    def _():
        spread_solved(start, solved, landed, p1_send, p1_recv)
        landed[tile_rows(local_tile), tile_cols(local_tile)] = solved[j]

    @pl.when(owner)
    def _():
        my_damping = 1.0 / (1.0 + COARSEN * full[REACTION, my_rows, my_cols])
        gathered_adj[j] = full[ADJOINT, my_rows, my_cols]
        await_gather(source_adjoint, gathered_adj, m2_send, m2_recv)

        def body(i, carry):
            k = T - 1 - i
            state, before, through = carry
            state = my_damping * state + gathered_adj[k]
            solved_adj[k] = state
            return (state, through, through + state)

        head = gathered_adj[T - 1]
        solved_adj[T - 1] = head
        _, before, through = lax.fori_loop(1, T, body, (head,) * 3)
        for slot, value in ((SUM_EXIT, before), (SUM_ADJOINT, through)):
            packed_adj[slot - SUM_EXIT] = value
            sums[slot, my_rows, my_cols] = value
        spread_sums(start, packed_adj, SUM_EXIT, 2, b2_send, b2_recv)

    @pl.when(holds_output)
    def _():
        spread_solved(start, solved_adj, landed_adj, p2_send, p2_recv)
        landed_adj[tile_rows(local_tile), tile_cols(local_tile)] = solved_adj[j]

    await_sums(packed, SUM_ENTRY, 3, b1_send, b1_recv)
    entry_sum = zipped(lambda a, c: a + c, get(sums, SUM_ENTRY), get(full, INITIAL))
    forward_points(entry_sum, float(T))
    await_solved(solved, landed, p1_send, p1_recv)
    states_out[0] = landed[...]

    await_sums(packed_adj, SUM_EXIT, 2, b2_send, b2_recv)
    g = adjoint_step(misfit_added(get(sums, SUM_EXIT), get(sums, SUM_STATES), get(sums, SUM_TARGET)))
    put(total, zipped(lambda a, c: a + c, get(sums, SUM_ADJOINT), g))

    def final_body(i, g):
        g = adjoint_points(g, (sums, SUM_TARGET))(i, g)
        put(total, zipped(lambda a, c: a + c, get(total), g))
        return g

    lax.fori_loop(0, COARSEN - 2, final_body, g)
    gradient_out[...] = total[own, :] * (1.0 / (COARSEN * T))
    await_solved(solved_adj, landed_adj, p2_send, p2_recv)
    adjoints_out[0] = landed_adj[...]

    input_sends(finish)
    scatter(finish, source_forward, gathered, m1_send, m1_recv)
    scatter(finish, source_adjoint, gathered_adj, m2_send, m2_recv)

    @pl.when(owner)
    def _():
        spread_sums(finish, packed, SUM_ENTRY, 3, b1_send, b1_recv)
        spread_sums(finish, packed_adj, SUM_EXIT, 2, b2_send, b2_recv)

    @pl.when(holds_output)
    def _():
        spread_solved(finish, solved, landed, p1_send, p1_recv)
        spread_solved(finish, solved_adj, landed_adj, p2_send, p2_recv)


def solution(mesh):
    T, X = mesh.shape["tm"], mesh.shape["space"]

    def shards(control, initial, diffusion, reaction, forward_guess, adjoint_guess, observed):
        rows, cols = control.shape
        grid_rows = rows * X
        tiles = (grid_rows // SUB) * (cols // LANES)
        own_tiles = (rows // SUB) * (cols // LANES)
        vmem = pl.BlockSpec(memory_space=pltpu.VMEM)
        f32 = lambda *shape: pltpu.VMEM(shape, jnp.float32)
        dma = lambda *shape: pltpu.SemaphoreType.DMA(shape)
        return pl.pallas_call(
            functools.partial(kernel, T, X),
            out_shape=(
                jax.ShapeDtypeStruct(forward_guess.shape, jnp.float32),
                jax.ShapeDtypeStruct(forward_guess.shape, jnp.float32),
                jax.ShapeDtypeStruct(control.shape, jnp.float32),
            ),
            in_specs=[vmem] * 7,
            out_specs=(vmem,) * 3,
            scratch_shapes=[
                f32(SLOTS, grid_rows, cols),
                f32(grid_rows, cols),
                f32(grid_rows, cols),
                f32(COARSEN - 1, grid_rows, cols),
                f32(grid_rows, cols),
                f32(5, grid_rows, cols),
                f32(T, 2, SUB, LANES),
                f32(T, SUB, LANES),
                f32(T, SUB, LANES),
                f32(T, SUB, LANES),
                f32(3, SUB, LANES),
                f32(2, SUB, LANES),
                f32(rows, cols),
                f32(rows, cols),
                dma(SLOTS, X), dma(SLOTS, X),
                dma(tiles), dma(T), dma(tiles), dma(T),
                dma(T), dma(tiles), dma(T), dma(tiles),
                dma(T), dma(own_tiles), dma(T), dma(own_tiles),
            ],
            compiler_params=pltpu.CompilerParams(collective_id=0, has_side_effects=True),
        )(control, initial, diffusion, reaction, forward_guess, adjoint_guess, observed)

    return jax.shard_map(
        shards,
        mesh=mesh,
        in_specs=(
            P("space", None),
            P("space", None),
            P("space", None),
            P("space", None),
            P("tm", "space", None),
            P("tm", "space", None),
            P("tm", "space", None),
        ),
        out_specs=(P("tm", "space", None), P("tm", "space", None), P("space", None)),
        check_vma=False,
    )
```

```python
import functools

import jax
import jax.numpy as jnp
from jax import lax
from jax.experimental import pallas as pl
from jax.experimental.pallas import tpu as pltpu
from jax.sharding import PartitionSpec as P

SWEEPS = 3
COARSEN = 8
SUB, LANES = 8, 128
MESH = pl.DeviceIdType.MESH

CONTROL, DIFFUSION, REACTION, ENTRY, GUESS, TARGET, FORWARD, EXIT, INITIAL, ADJOINT = range(10)
SLOTS = 10
SUM_TARGET, SUM_ENTRY, SUM_EXIT = range(3)
SUMS = 3


def kernel(
    T, X,
    control_ref, initial_ref, diffusion_ref, reaction_ref, guess_ref, adjoint_ref, observed_ref,
    states_out, adjoints_out, gradient_out,
    full, own_adjoint, weight, inverse, points, total, sums,
    gathered_target, gathered, gathered_adj, solved, solved_adj, packed, landed, landed_adj,
    local_sem, reach, in_send, in_recv, m0_send, m0_recv, m1_send, m1_recv, m2_send, m2_recv,
    b0_send, b0_recv, b1_send, b1_recv, b2_send, b2_recv, p1_send, p1_recv, p2_send, p2_recv,
):
    rows, cols = control_ref.shape
    grid_rows = rows * X
    col_tiles = cols // LANES
    tiles = (grid_rows // SUB) * col_tiles
    own_tiles = (rows // SUB) * col_tiles
    stride = T // tiles
    j = lax.axis_index("tm")
    x = lax.axis_index("space")
    first, last = j == 0, j == T - 1

    def device(tm, space):
        return {"tm": tm, "space": space}

    def side(o):
        return lax.rem(x + o, X)

    def from_side(o):
        return lax.rem(x + X - o, X)

    def block_rows(space):
        return pl.ds(pl.multiple_of(space * rows, rows), rows)

    own = block_rows(x)

    barrier = pltpu.get_barrier_semaphore()

    def greet(tm, space):
        pl.semaphore_signal(barrier, inc=1, device_id=device(tm, space), device_id_type=MESH)

    for o in range(1, X):
        greet(j, side(o))
    for o in range(X):
        @pl.when(j > 0)
        def _():
            greet(j - 1, side(o))

        @pl.when(j < T - 1)
        def _():
            greet(j + 1, side(o))

    loads = [
        pltpu.make_async_copy(src, dst, local_sem.at[n])
        for n, (src, dst) in enumerate((
            (diffusion_ref, full.at[DIFFUSION, own, :]),
            (reaction_ref, full.at[REACTION, own, :]),
            (control_ref, full.at[CONTROL, own, :]),
            (guess_ref.at[0], full.at[GUESS, own, :]),
            (observed_ref.at[0], full.at[TARGET, own, :]),
            (adjoint_ref.at[0], own_adjoint),
            (initial_ref, full.at[INITIAL, own, :]),
        ))
    ]
    entry_load = pltpu.make_async_copy(initial_ref, full.at[ENTRY, own, :], local_sem.at[len(loads)])

    for copy in loads:
        copy.start()

    @pl.when(first)
    def _():
        entry_load.start()

    @pl.when(last)
    def _():
        full[EXIT] = jnp.zeros((grid_rows, cols), jnp.float32)

    for copy in loads:
        copy.wait()

    @pl.when(first)
    def _():
        entry_load.wait()

    neighbours_count = (j > 0).astype(jnp.int32) + (j < T - 1).astype(jnp.int32)
    pl.semaphore_wait(barrier, (X - 1) + X * neighbours_count)

    rounds = (T - 2).bit_length()

    def reach_out(r):
        h = 1 << r

        @pl.when(j >= h)
        def _():
            pl.semaphore_signal(reach.at[r], inc=1, device_id=device(j - h, x), device_id_type=MESH)

        @pl.when(j < T - h)
        def _():
            pl.semaphore_signal(reach.at[r], inc=1, device_id=device(j + h, x), device_id_type=MESH)

    def reached(r):
        h = 1 << r
        pl.semaphore_wait(reach.at[r], (j >= h).astype(jnp.int32) + (j < T - h).astype(jnp.int32))

    def send(src, slot, o, tm):
        return pltpu.make_async_remote_copy(
            src_ref=src, dst_ref=full.at[slot, own, :],
            send_sem=in_send.at[slot, o], recv_sem=in_recv.at[slot, o],
            device_id=device(tm, side(o)), device_id_type=MESH,
        )

    def mine_of(slot):
        return full.at[slot, own, :]

    def initial_entry_copy(o):
        return pltpu.make_async_remote_copy(
            src_ref=mine_of(INITIAL), dst_ref=full.at[ENTRY, own, :],
            send_sem=in_send.at[FORWARD, o], recv_sem=in_recv.at[ENTRY, o],
            device_id=device(j, side(o)), device_id_type=MESH,
        )

    def input_sends(act):
        for o in range(1, X):
            for slot in (DIFFUSION, REACTION, CONTROL):
                act(send(mine_of(slot), slot, o, j))

            @pl.when(first)
            def _():
                act(initial_entry_copy(o))

        @pl.when(j < T - 1)
        def _():
            for o in range(X):
                act(send(mine_of(GUESS), ENTRY, o, j + 1))

        for o in range(1, X):
            for slot in (TARGET, GUESS):
                act(send(mine_of(slot), slot, o, j))

        @pl.when(j > 0)
        def _():
            for o in range(X):
                act(send(own_adjoint, EXIT, o, j - 1))

        for o in range(1, X):
            act(send(mine_of(INITIAL), INITIAL, o, j))

    def await_input(slot, o):
        pltpu.make_async_remote_copy(
            src_ref=own_adjoint, dst_ref=full.at[slot, block_rows(from_side(o)), :],
            send_sem=in_send.at[slot, o], recv_sem=in_recv.at[slot, o],
            device_id=device(j, side(o)), device_id_type=MESH,
        ).wait_recv()

    input_sends(lambda copy: copy.start())
    reach_out(0)

    lane = lax.broadcasted_iota(jnp.int32, (grid_rows, LANES), 1)
    row = lax.broadcasted_iota(jnp.int32, (grid_rows, LANES), 0)
    lane_low, lane_high = lane == 0, lane == LANES - 1
    row_low, row_high = row == 0, row == grid_rows - 1
    blocks = range(col_tiles)
    zero = jnp.zeros((grid_rows, LANES), jnp.float32)

    def cut(value):
        return [value[:, b * LANES : (b + 1) * LANES] for b in blocks]

    def get(ref, *index):
        return [ref[(*index, slice(None), pl.ds(b * LANES, LANES))] for b in blocks]

    def put(ref, value, *index):
        for b in blocks:
            ref[(*index, slice(None), pl.ds(b * LANES, LANES))] = value[b]

    def zipped(f, *lists):
        return [f(*items) for items in zip(*lists)]

    def neighbours(v):
        right = [pltpu.roll(b, LANES - 1, 1) for b in v]
        left = [pltpu.roll(b, 1, 1) for b in v]
        out = []
        for b in blocks:
            up = jnp.where(row_low, 0.0, pltpu.roll(v[b], 1, 0))
            down = jnp.where(row_high, 0.0, pltpu.roll(v[b], grid_rows - 1, 0))
            to_right = jnp.where(lane_high, right[b + 1] if b + 1 < col_tiles else zero, right[b])
            to_left = jnp.where(lane_low, left[b - 1] if b > 0 else zero, left[b])
            out.append((up + down) + (to_right + to_left))
        return out

    def forward_step(v, scale):
        rhs = zipped(lambda a, c: a + scale * c, v, get(full, CONTROL))
        w = get(weight)
        base = zipped(lambda a, c: a * c, rhs, get(inverse))
        iterate = rhs
        for _ in range(SWEEPS):
            iterate = zipped(lambda a, c, n: a + c * n, base, w, neighbours(iterate))
        return iterate

    def adjoint_step(y):
        w = get(weight)
        carried, summed = y, y
        for _ in range(SWEEPS - 1):
            carried = neighbours(zipped(lambda a, c: a * c, w, carried))
            summed = zipped(lambda a, c: a + c, summed, carried)
        tail = neighbours(zipped(lambda a, c: a * c, w, carried))
        return zipped(lambda a, c, t: a * c + t, summed, get(inverse), tail)

    def misfit_added(g, point, target):
        return zipped(lambda a, p, o: a + (p - o) * (1.0 / COARSEN), g, point, target)

    for o in range(1, X):
        await_input(DIFFUSION, o)
        await_input(REACTION, o)
    reached(0)
    if rounds > 1:
        reach_out(1)
    spread = full[DIFFUSION]
    diagonal = 1.0 + 4.0 * spread + full[REACTION]
    reciprocal = 1.0 / diagonal
    inverse[...] = reciprocal
    weight[...] = spread * reciprocal

    def tile_rows(d):
        return pl.ds(pl.multiple_of((d // col_tiles) * SUB, SUB), SUB)

    def tile_cols(d):
        return pl.ds(pl.multiple_of(lax.rem(d, col_tiles) * LANES, LANES), LANES)

    mine = j // stride
    owner = jnp.logical_and(lax.rem(j, stride) == 0, mine < tiles)
    my_rows, my_cols = tile_rows(lax.rem(mine, tiles)), tile_cols(lax.rem(mine, tiles))

    def scatter(act, slot, target, send_sem, recv_sem):
        def body(i, c):
            d = lax.rem(mine + i, tiles)

            @pl.when(d * stride != j)
            def _():
                act(pltpu.make_async_remote_copy(
                    src_ref=full.at[slot, tile_rows(d), tile_cols(d)], dst_ref=target.at[j],
                    send_sem=send_sem.at[d], recv_sem=recv_sem.at[j],
                    device_id=device(d * stride, x), device_id_type=MESH,
                ))

            return c

        lax.fori_loop(0, tiles, body, 0)

    def await_gather(slot, target, send_sem, recv_sem):
        target[j] = full[slot, my_rows, my_cols]

        def body(i, c):
            k = lax.rem(j + i, T)
            pltpu.make_async_remote_copy(
                src_ref=full.at[slot, my_rows, my_cols], dst_ref=target.at[k],
                send_sem=send_sem.at[0], recv_sem=recv_sem.at[k],
                device_id=device(k, x), device_id_type=MESH,
            ).wait_recv()
            return c

        lax.fori_loop(1, T, body, 0)

    def spread_sums(act, slot, send_sem, recv_sem):
        def body(i, c):
            k = lax.rem(j + i, T)
            act(pltpu.make_async_remote_copy(
                src_ref=packed.at[slot], dst_ref=sums.at[slot, my_rows, my_cols],
                send_sem=send_sem.at[k], recv_sem=recv_sem.at[mine],
                device_id=device(k, x), device_id_type=MESH,
            ))
            return c

        lax.fori_loop(1, T, body, 0)

    def await_sums(slot, send_sem, recv_sem):
        def body(d, c):
            @pl.when(d * stride != j)
            def _():
                pltpu.make_async_remote_copy(
                    src_ref=packed.at[slot], dst_ref=sums.at[slot, tile_rows(d), tile_cols(d)],
                    send_sem=send_sem.at[0], recv_sem=recv_sem.at[d],
                    device_id=device(d * stride, x), device_id_type=MESH,
                ).wait_recv()

            return c

        lax.fori_loop(0, tiles, body, 0)

    local = mine - x * own_tiles
    holds_output = jnp.logical_and(owner, jnp.logical_and(local >= 0, local < own_tiles))
    local_tile = lax.rem(local + tiles, own_tiles)

    def spread_solved(act, source, landing, send_sem, recv_sem):
        def body(i, c):
            k = lax.rem(j + i, T)
            act(pltpu.make_async_remote_copy(
                src_ref=source.at[k], dst_ref=landing(local_tile),
                send_sem=send_sem.at[k], recv_sem=recv_sem.at[local_tile],
                device_id=device(k, x), device_id_type=MESH,
            ))
            return c

        lax.fori_loop(1, T, body, 0)

    def await_solved(source, landing, send_sem, recv_sem):
        def body(d, c):
            source_tm = (d + x * own_tiles) * stride

            @pl.when(source_tm != j)
            def _():
                pltpu.make_async_remote_copy(
                    src_ref=source.at[0], dst_ref=landing(d),
                    send_sem=send_sem.at[0], recv_sem=recv_sem.at[d],
                    device_id=device(source_tm, x), device_id_type=MESH,
                ).wait_recv()

            return c

        lax.fori_loop(0, own_tiles, body, 0)

    def landing(d):
        return landed.at[tile_rows(d), tile_cols(d)]

    def landing_adj(d):
        return landed_adj.at[:, tile_rows(d), tile_cols(d)]

    start = lambda copy: copy.start()
    finish = lambda copy: copy.wait_send()

    def forward_points(start, scale, beside=None):
        def body(i, v):
            v = forward_step(v, scale)
            put(points, v, i)
            if beside is not None:
                beside(i)
            return v

        return lax.fori_loop(0, COARSEN - 1, body, start)

    for o in range(1, X):
        await_input(CONTROL, o)
        await_input(ENTRY, o)

    @pl.when(j > 0)
    def _():
        await_input(ENTRY, 0)

    if rounds > 1:
        reached(1)
    if rounds > 2:
        reach_out(2)
    damping = 1.0 / (1.0 + COARSEN * full[REACTION])
    share_at = 3

    def beside_forward(i):
        for r in range(3, rounds):
            @pl.when(i == ((r - 3) * share_at) // (rounds - 3))
            def _():
                reached(r - 1)
                reach_out(r)

        @pl.when(i == share_at)
        def _():
            if rounds > 2:
                reached(rounds - 1)
            for o in range(1, X):
                await_input(TARGET, o)
            scatter(start, TARGET, gathered_target, m0_send, m0_recv)

    v = forward_points(get(full, ENTRY), 1.0, beside_forward)
    v = forward_step(v, 1.0)
    keep = (j > 0).astype(jnp.float32)
    put(full, zipped(lambda a, d, s: a - keep * (d * s), v, cut(damping), get(full, ENTRY)), FORWARD)
    scatter(start, FORWARD, gathered, m1_send, m1_recv)

    for o in range(1, X):
        await_input(GUESS, o)
        await_input(INITIAL, o)

    @pl.when(j < T - 1)
    def _():
        for o in range(X):
            await_input(EXIT, o)

    def adjoint_points(g, target):
        def body(i, g):
            at = COARSEN - 2 - i
            return adjoint_step(misfit_added(g, get(points, at), get(*target)))

        return body

    g = adjoint_step(misfit_added(get(full, EXIT), get(full, GUESS), get(full, TARGET)))
    g = lax.fori_loop(0, COARSEN - 1, adjoint_points(g, (full, TARGET)), g)
    put(full, zipped(lambda a, d, t: a - d * t, g, cut(damping), get(full, EXIT)), ADJOINT)
    scatter(start, ADJOINT, gathered_adj, m2_send, m2_recv)

    @pl.when(owner)
    def _():
        def share(slot, value, send_sem, recv_sem):
            packed[slot] = value
            sums[slot, my_rows, my_cols] = value
            spread_sums(start, slot, send_sem, recv_sem)

        my_damping = 1.0 / (1.0 + COARSEN * full[REACTION, my_rows, my_cols])

        await_gather(TARGET, gathered_target, m0_send, m0_recv)
        target = lax.fori_loop(1, T, lambda k, c: c + gathered_target[k], gathered_target[0])
        share(SUM_TARGET, target, b0_send, b0_recv)

        await_gather(FORWARD, gathered, m1_send, m1_recv)

        def forward_body(k, carry):
            state, before, through = carry
            state = my_damping * state + gathered[k]
            solved[k] = state
            return (state, through, through + state)

        head = gathered[0]
        solved[0] = head
        _, before, states = lax.fori_loop(1, T, forward_body, (head,) * 3)
        share(SUM_ENTRY, before, b1_send, b1_recv)

        await_gather(ADJOINT, gathered_adj, m2_send, m2_recv)

        def adjoint_body(i, carry):
            k = T - 1 - i
            state, before, through = carry
            state = my_damping * state + gathered_adj[k]
            solved_adj[k, 0] = state
            return (state, through, through + state)

        head = gathered_adj[T - 1]
        solved_adj[T - 1, 0] = head
        _, before, adjoints = lax.fori_loop(1, T, adjoint_body, (head,) * 3)
        share(SUM_EXIT, before + (states - target) * (1.0 / COARSEN), b2_send, b2_recv)

        def fill(k, c):
            solved_adj[k, 1] = adjoints
            return c

        lax.fori_loop(0, T, fill, 0)

    @pl.when(holds_output)
    def _():
        spread_solved(start, solved_adj, landing_adj, p2_send, p2_recv)
        spread_solved(start, solved, landing, p1_send, p1_recv)
        landed_adj[:, tile_rows(local_tile), tile_cols(local_tile)] = solved_adj[j]
        landed[tile_rows(local_tile), tile_cols(local_tile)] = solved[j]

    await_sums(SUM_ENTRY, b1_send, b1_recv)
    entry_sum = zipped(lambda a, c: a + c, get(sums, SUM_ENTRY), get(full, INITIAL))
    forward_points(entry_sum, float(T))

    await_sums(SUM_TARGET, b0_send, b0_recv)
    await_sums(SUM_EXIT, b2_send, b2_recv)
    g = adjoint_step(get(sums, SUM_EXIT))
    put(total, g)

    def final_body(i, g):
        g = adjoint_points(g, (sums, SUM_TARGET))(i, g)
        put(total, zipped(lambda a, c: a + c, get(total), g))
        return g

    lax.fori_loop(0, COARSEN - 2, final_body, g)
    await_solved(solved_adj, landing_adj, p2_send, p2_recv)
    gradient_out[...] = (landed_adj[1] + total[own, :]) * (1.0 / (COARSEN * T))
    adjoints_out[0] = landed_adj[0]
    await_solved(solved, landing, p1_send, p1_recv)
    states_out[0] = landed[...]

    input_sends(finish)
    scatter(finish, TARGET, gathered_target, m0_send, m0_recv)
    scatter(finish, FORWARD, gathered, m1_send, m1_recv)
    scatter(finish, ADJOINT, gathered_adj, m2_send, m2_recv)

    @pl.when(owner)
    def _():
        spread_sums(finish, SUM_TARGET, b0_send, b0_recv)
        spread_sums(finish, SUM_ENTRY, b1_send, b1_recv)
        spread_sums(finish, SUM_EXIT, b2_send, b2_recv)

    @pl.when(holds_output)
    def _():
        spread_solved(finish, solved_adj, landing_adj, p2_send, p2_recv)
        spread_solved(finish, solved, landing, p1_send, p1_recv)


def emit(*refs):
    for source, target in zip(refs[:3], refs[3:]):
        target[...] = source[...]


def solution(mesh):
    T, X = mesh.shape["tm"], mesh.shape["space"]

    def shards(control, initial, diffusion, reaction, forward_guess, adjoint_guess, observed):
        rows, cols = control.shape
        grid_rows = rows * X
        tiles = (grid_rows // SUB) * (cols // LANES)
        own_tiles = (rows // SUB) * (cols // LANES)
        vmem = pl.BlockSpec(memory_space=pltpu.VMEM)
        f32 = lambda *shape: pltpu.VMEM(shape, jnp.float32)
        dma = lambda *shape: pltpu.SemaphoreType.DMA(shape)
        outs = pl.pallas_call(
            functools.partial(kernel, T, X),
            out_shape=(
                jax.ShapeDtypeStruct(forward_guess.shape, jnp.float32),
                jax.ShapeDtypeStruct(forward_guess.shape, jnp.float32),
                jax.ShapeDtypeStruct(control.shape, jnp.float32),
            ),
            in_specs=[pl.BlockSpec(memory_space=pl.ANY)] * 7,
            out_specs=(vmem,) * 3,
            scratch_shapes=[
                f32(SLOTS, grid_rows, cols),
                f32(rows, cols),
                f32(grid_rows, cols),
                f32(grid_rows, cols),
                f32(COARSEN - 1, grid_rows, cols),
                f32(grid_rows, cols),
                f32(SUMS, grid_rows, cols),
                f32(T, SUB, LANES),
                f32(T, SUB, LANES),
                f32(T, SUB, LANES),
                f32(T, SUB, LANES),
                f32(T, 2, SUB, LANES),
                f32(SUMS, SUB, LANES),
                f32(rows, cols),
                f32(2, rows, cols),
                dma(8),
                pltpu.SemaphoreType.REGULAR(((T - 2).bit_length(),)),
                dma(SLOTS, X), dma(SLOTS, X),
                dma(tiles), dma(T), dma(tiles), dma(T), dma(tiles), dma(T),
                dma(T), dma(tiles), dma(T), dma(tiles), dma(T), dma(tiles),
                dma(T), dma(own_tiles), dma(T), dma(own_tiles),
            ],
            compiler_params=pltpu.CompilerParams(collective_id=0, has_side_effects=True),
        )(control, initial, diffusion, reaction, forward_guess, adjoint_guess, observed)
        return pl.pallas_call(
            emit,
            out_shape=tuple(jax.ShapeDtypeStruct(out.shape, out.dtype) for out in outs),
            in_specs=[vmem] * 3,
            out_specs=(vmem,) * 3,
        )(*outs)

    return jax.shard_map(
        shards,
        mesh=mesh,
        in_specs=(
            P("space", None),
            P("space", None),
            P("space", None),
            P("space", None),
            P("tm", "space", None),
            P("tm", "space", None),
            P("tm", "space", None),
        ),
        out_specs=(P("tm", "space", None), P("tm", "space", None), P("space", None)),
        check_vma=False,
    )
```

```python
import functools

import jax
import jax.numpy as jnp
from jax import lax
from jax.experimental import pallas as pl
from jax.experimental.pallas import tpu as pltpu
from jax.sharding import PartitionSpec as P

SWEEPS = 3
COARSEN = 8
SUB, LANES = 8, 128
MESH = pl.DeviceIdType.MESH

CONTROL, DIFFUSION, REACTION, ENTRY, GUESS, TARGET, FORWARD, EXIT, INITIAL, ADJOINT = range(10)
SLOTS = 10
SUM_TARGET, SUM_ENTRY, SUM_EXIT = range(3)
SUMS = 3


def kernel(
    T, X,
    control_ref, initial_ref, diffusion_ref, reaction_ref, guess_ref, adjoint_ref, observed_ref,
    states_out, adjoints_out, gradient_out,
    full, own_adjoint, weight, inverse, points, total, sums,
    gathered_target, gathered, gathered_adj, solved, solved_adj, packed, landed, landed_adj,
    local_sem, reach, in_send, in_recv, m0, m1, m2,
    b0, b1, b2, p1, p2,
):
    rows, cols = control_ref.shape
    grid_rows = rows * X
    col_tiles = cols // LANES
    tiles = (grid_rows // SUB) * col_tiles
    own_tiles = (rows // SUB) * col_tiles
    stride = T // tiles
    j = lax.axis_index("tm")
    x = lax.axis_index("space")
    first, last = j == 0, j == T - 1

    def device(tm, space):
        return {"tm": tm, "space": space}

    def side(o):
        return lax.rem(x + o, X)

    def from_side(o):
        return lax.rem(x + X - o, X)

    def block_rows(space):
        return pl.ds(pl.multiple_of(space * rows, rows), rows)

    own = block_rows(x)

    barrier = pltpu.get_barrier_semaphore()

    def greet(tm, space):
        pl.semaphore_signal(barrier, inc=1, device_id=device(tm, space), device_id_type=MESH)

    for o in range(1, X):
        greet(j, side(o))
    for o in range(X):
        @pl.when(j > 0)
        def _():
            greet(j - 1, side(o))

        @pl.when(j < T - 1)
        def _():
            greet(j + 1, side(o))

    loads = [
        pltpu.make_async_copy(src, dst, local_sem.at[n])
        for n, (src, dst) in enumerate((
            (diffusion_ref, full.at[DIFFUSION, own, :]),
            (reaction_ref, full.at[REACTION, own, :]),
            (control_ref, full.at[CONTROL, own, :]),
            (guess_ref.at[0], full.at[GUESS, own, :]),
            (observed_ref.at[0], full.at[TARGET, own, :]),
            (adjoint_ref.at[0], own_adjoint),
            (initial_ref, full.at[INITIAL, own, :]),
        ))
    ]
    entry_load = pltpu.make_async_copy(initial_ref, full.at[ENTRY, own, :], local_sem.at[len(loads)])

    for copy in loads:
        copy.start()

    @pl.when(first)
    def _():
        entry_load.start()

    @pl.when(last)
    def _():
        full[EXIT] = jnp.zeros((grid_rows, cols), jnp.float32)

    for copy in loads:
        copy.wait()

    @pl.when(first)
    def _():
        entry_load.wait()

    neighbours_count = (j > 0).astype(jnp.int32) + (j < T - 1).astype(jnp.int32)
    pl.semaphore_wait(barrier, (X - 1) + X * neighbours_count)

    rounds = (T - 2).bit_length()

    def reach_out(r):
        h = 1 << r

        @pl.when(j >= h)
        def _():
            pl.semaphore_signal(reach.at[r], inc=1, device_id=device(j - h, x), device_id_type=MESH)

        @pl.when(j < T - h)
        def _():
            pl.semaphore_signal(reach.at[r], inc=1, device_id=device(j + h, x), device_id_type=MESH)

    def reached(r):
        h = 1 << r
        pl.semaphore_wait(reach.at[r], (j >= h).astype(jnp.int32) + (j < T - h).astype(jnp.int32))

    def send(src, slot, o, tm):
        return pltpu.make_async_remote_copy(
            src_ref=src, dst_ref=full.at[slot, own, :],
            send_sem=in_send.at[slot, o], recv_sem=in_recv.at[slot, o],
            device_id=device(tm, side(o)), device_id_type=MESH,
        )

    def mine_of(slot):
        return full.at[slot, own, :]

    def initial_entry_copy(o):
        return pltpu.make_async_remote_copy(
            src_ref=mine_of(INITIAL), dst_ref=full.at[ENTRY, own, :],
            send_sem=in_send.at[FORWARD, o], recv_sem=in_recv.at[ENTRY, o],
            device_id=device(j, side(o)), device_id_type=MESH,
        )

    def input_sends(act):
        for o in range(1, X):
            for slot in (DIFFUSION, REACTION, CONTROL):
                act(send(mine_of(slot), slot, o, j))

            @pl.when(first)
            def _():
                act(initial_entry_copy(o))

        @pl.when(j < T - 1)
        def _():
            for o in range(X):
                act(send(mine_of(GUESS), ENTRY, o, j + 1))

        for o in range(1, X):
            for slot in (TARGET, GUESS):
                act(send(mine_of(slot), slot, o, j))

        @pl.when(j > 0)
        def _():
            for o in range(X):
                act(send(own_adjoint, EXIT, o, j - 1))

        for o in range(1, X):
            act(send(mine_of(INITIAL), INITIAL, o, j))

    def await_input(slot, o):
        pltpu.make_async_remote_copy(
            src_ref=own_adjoint, dst_ref=full.at[slot, block_rows(from_side(o)), :],
            send_sem=in_send.at[slot, o], recv_sem=in_recv.at[slot, o],
            device_id=device(j, side(o)), device_id_type=MESH,
        ).wait_recv()

    input_sends(lambda copy: copy.start())
    reach_out(0)

    lane = lax.broadcasted_iota(jnp.int32, (grid_rows, LANES), 1)
    row = lax.broadcasted_iota(jnp.int32, (grid_rows, LANES), 0)
    lane_low, lane_high = lane == 0, lane == LANES - 1
    row_low, row_high = row == 0, row == grid_rows - 1
    blocks = range(col_tiles)
    zero = jnp.zeros((grid_rows, LANES), jnp.float32)

    def cut(value):
        return [value[:, b * LANES : (b + 1) * LANES] for b in blocks]

    def get(ref, *index):
        return [ref[(*index, slice(None), pl.ds(b * LANES, LANES))] for b in blocks]

    def put(ref, value, *index):
        for b in blocks:
            ref[(*index, slice(None), pl.ds(b * LANES, LANES))] = value[b]

    def zipped(f, *lists):
        return [f(*items) for items in zip(*lists)]

    def neighbours(v):
        right = [pltpu.roll(b, LANES - 1, 1) for b in v]
        left = [pltpu.roll(b, 1, 1) for b in v]
        out = []
        for b in blocks:
            up = jnp.where(row_low, 0.0, pltpu.roll(v[b], 1, 0))
            down = jnp.where(row_high, 0.0, pltpu.roll(v[b], grid_rows - 1, 0))
            to_right = jnp.where(lane_high, right[b + 1] if b + 1 < col_tiles else zero, right[b])
            to_left = jnp.where(lane_low, left[b - 1] if b > 0 else zero, left[b])
            out.append((up + down) + (to_right + to_left))
        return out

    def forward_step(v, scale):
        rhs = zipped(lambda a, c: a + scale * c, v, get(full, CONTROL))
        w = get(weight)
        base = zipped(lambda a, c: a * c, rhs, get(inverse))
        iterate = rhs
        for _ in range(SWEEPS):
            iterate = zipped(lambda a, c, n: a + c * n, base, w, neighbours(iterate))
        return iterate

    def adjoint_step(y):
        w = get(weight)
        carried, summed = y, y
        for _ in range(SWEEPS - 1):
            carried = neighbours(zipped(lambda a, c: a * c, w, carried))
            summed = zipped(lambda a, c: a + c, summed, carried)
        tail = neighbours(zipped(lambda a, c: a * c, w, carried))
        return zipped(lambda a, c, t: a * c + t, summed, get(inverse), tail)

    def misfit_added(g, point, target):
        return zipped(lambda a, p, o: a + (p - o) * (1.0 / COARSEN), g, point, target)

    for o in range(1, X):
        await_input(DIFFUSION, o)
        await_input(REACTION, o)
    reached(0)
    if rounds > 1:
        reach_out(1)
    spread = full[DIFFUSION]
    diagonal = 1.0 + 4.0 * spread + full[REACTION]
    reciprocal = 1.0 / diagonal
    inverse[...] = reciprocal
    weight[...] = spread * reciprocal

    def tile_rows(d):
        return pl.ds(pl.multiple_of((d // col_tiles) * SUB, SUB), SUB)

    def tile_cols(d):
        return pl.ds(pl.multiple_of(lax.rem(d, col_tiles) * LANES, LANES), LANES)

    mine = j // stride
    owner = jnp.logical_and(lax.rem(j, stride) == 0, mine < tiles)
    my_rows, my_cols = tile_rows(lax.rem(mine, tiles)), tile_cols(lax.rem(mine, tiles))

    ordered = T & (T - 1) == 0 and T <= 32
    flips = [(1 << n, (1 << n) * (1 - 2 * lax.rem(j // (1 << n), 2))) for n in range((T - 1).bit_length())]

    def each_other(f):
        if ordered:
            for i in range(T - 1, 0, -1):
                f(sum(flip for bit, flip in flips if i & bit) + j)
        else:
            def body(i, c):
                f(lax.rem(j + i, T))
                return c

            lax.fori_loop(1, T, body, 0)

    every_owner = tiles == T

    def each_owner(f):
        if every_owner:
            each_other(f)
        else:
            def body(i, c):
                d = lax.rem(mine + i, tiles)

                @pl.when(d * stride != j)
                def _():
                    f(d)

                return c

            lax.fori_loop(0, tiles, body, 0)

    def drained(buffer, sems, count, less, receive):
        def wait(n):
            ref = buffer.at[pl.ds(0, n)]
            copy = pltpu.make_async_remote_copy(
                src_ref=ref, dst_ref=ref, send_sem=sems.at[0], recv_sem=sems.at[1],
                device_id=device(lax.rem(j + 1, T), x), device_id_type=MESH,
            )
            if receive:
                copy.wait_recv()
            else:
                copy.wait_send()

        if less is True:
            wait(count - 1)
        else:
            pl.when(less)(lambda: wait(count - 1))
            pl.when(jnp.logical_not(less))(lambda: wait(count))

    is_owner = True if every_owner else owner

    def scatter(slot, target, sems):
        def one(d):
            pltpu.make_async_remote_copy(
                src_ref=full.at[slot, tile_rows(d), tile_cols(d)], dst_ref=target.at[j],
                send_sem=sems.at[0], recv_sem=sems.at[1],
                device_id=device(d * stride, x), device_id_type=MESH,
            ).start()

        each_owner(one)

    def scattered(target, sems):
        drained(target, sems, tiles, is_owner, False)

    def await_gather(slot, target, sems):
        target[j] = full[slot, my_rows, my_cols]
        drained(target, sems, T, True, True)

    def spread_sums(slot, sems):
        def one(k):
            pltpu.make_async_remote_copy(
                src_ref=packed.at[slot], dst_ref=sums.at[slot, my_rows, my_cols],
                send_sem=sems.at[0], recv_sem=sems.at[1],
                device_id=device(k, x), device_id_type=MESH,
            ).start()

        each_other(one)

    def sums_spread(sems):
        drained(gathered, sems, T, True, False)

    def await_sums(sems):
        drained(gathered, sems, tiles, is_owner, True)

    local = mine - x * own_tiles
    holds_output = jnp.logical_and(owner, jnp.logical_and(local >= 0, local < own_tiles))
    local_tile = lax.rem(local + tiles, own_tiles)

    def spread_solved(source, landing, sems):
        def one(k):
            pltpu.make_async_remote_copy(
                src_ref=source.at[k], dst_ref=landing(local_tile),
                send_sem=sems.at[0], recv_sem=sems.at[1],
                device_id=device(k, x), device_id_type=MESH,
            ).start()

        each_other(one)

    def solved_spread(source, sems):
        drained(source, sems, T, True, False)

    def await_solved(source, sems):
        drained(source, sems, own_tiles, holds_output, True)

    def landing(d):
        return landed.at[tile_rows(d), tile_cols(d)]

    def landing_adj(d):
        return landed_adj.at[:, tile_rows(d), tile_cols(d)]


    def forward_points(start, scale, beside=None):
        def body(i, v):
            v = forward_step(v, scale)
            put(points, v, i)
            if beside is not None:
                beside(i)
            return v

        return lax.fori_loop(0, COARSEN - 1, body, start)

    for o in range(1, X):
        await_input(CONTROL, o)
        await_input(ENTRY, o)

    @pl.when(j > 0)
    def _():
        await_input(ENTRY, 0)

    if rounds > 1:
        reached(1)
    if rounds > 2:
        reach_out(2)
    damping = 1.0 / (1.0 + COARSEN * full[REACTION])
    share_at = 3

    def beside_forward(i):
        for r in range(3, rounds):
            @pl.when(i == ((r - 3) * share_at) // (rounds - 3))
            def _():
                reached(r - 1)
                reach_out(r)

        @pl.when(i == share_at)
        def _():
            if rounds > 2:
                reached(rounds - 1)
            for o in range(1, X):
                await_input(TARGET, o)
            scatter(TARGET, gathered_target, m0)

    v = forward_points(get(full, ENTRY), 1.0, beside_forward)
    v = forward_step(v, 1.0)
    keep = (j > 0).astype(jnp.float32)
    put(full, zipped(lambda a, d, s: a - keep * (d * s), v, cut(damping), get(full, ENTRY)), FORWARD)
    scatter(FORWARD, gathered, m1)

    for o in range(1, X):
        await_input(GUESS, o)
        await_input(INITIAL, o)

    @pl.when(j < T - 1)
    def _():
        for o in range(X):
            await_input(EXIT, o)

    def adjoint_points(g, target):
        def body(i, g):
            at = COARSEN - 2 - i
            return adjoint_step(misfit_added(g, get(points, at), get(*target)))

        return body

    g = adjoint_step(misfit_added(get(full, EXIT), get(full, GUESS), get(full, TARGET)))
    g = lax.fori_loop(0, COARSEN - 1, adjoint_points(g, (full, TARGET)), g)
    put(full, zipped(lambda a, d, t: a - d * t, g, cut(damping), get(full, EXIT)), ADJOINT)
    scatter(ADJOINT, gathered_adj, m2)

    @pl.when(owner)
    def _():
        def share(slot, value, sems):
            packed[slot] = value
            sums[slot, my_rows, my_cols] = value
            spread_sums(slot, sems)

        my_damping = 1.0 / (1.0 + COARSEN * full[REACTION, my_rows, my_cols])

        await_gather(TARGET, gathered_target, m0)
        target = lax.fori_loop(1, T, lambda k, c: c + gathered_target[k], gathered_target[0])
        share(SUM_TARGET, target, b0)

        await_gather(FORWARD, gathered, m1)

        def forward_body(k, carry):
            state, before, through = carry
            state = my_damping * state + gathered[k]
            solved[k] = state
            return (state, through, through + state)

        head = gathered[0]
        solved[0] = head
        _, before, states = lax.fori_loop(1, T, forward_body, (head,) * 3)
        share(SUM_ENTRY, before, b1)

        await_gather(ADJOINT, gathered_adj, m2)

        def adjoint_body(i, carry):
            k = T - 1 - i
            state, before, through = carry
            state = my_damping * state + gathered_adj[k]
            solved_adj[k, 0] = state
            return (state, through, through + state)

        head = gathered_adj[T - 1]
        solved_adj[T - 1, 0] = head
        _, before, adjoints = lax.fori_loop(1, T, adjoint_body, (head,) * 3)
        share(SUM_EXIT, before + (states - target) * (1.0 / COARSEN), b2)

        def fill(k, c):
            solved_adj[k, 1] = adjoints
            return c

        lax.fori_loop(0, T, fill, 0)

    @pl.when(holds_output)
    def _():
        spread_solved(solved_adj, landing_adj, p2)
        spread_solved(solved, landing, p1)
        landed_adj[:, tile_rows(local_tile), tile_cols(local_tile)] = solved_adj[j]
        landed[tile_rows(local_tile), tile_cols(local_tile)] = solved[j]

    await_sums(b1)
    entry_sum = zipped(lambda a, c: a + c, get(sums, SUM_ENTRY), get(full, INITIAL))
    forward_points(entry_sum, float(T))

    await_sums(b0)
    input_sends(lambda copy: copy.wait_send())
    scattered(gathered_target, m0)
    scattered(gathered, m1)
    scattered(gathered_adj, m2)

    @pl.when(owner)
    def _():
        sums_spread(b0)
        sums_spread(b1)

    await_sums(b2)
    g = adjoint_step(get(sums, SUM_EXIT))
    put(total, g)

    def final_body(i, g):
        g = adjoint_points(g, (sums, SUM_TARGET))(i, g)
        put(total, zipped(lambda a, c: a + c, get(total), g))
        return g

    lax.fori_loop(0, COARSEN - 2, final_body, g)
    await_solved(solved_adj, p2)
    gradient_out[...] = (landed_adj[1] + total[own, :]) * (1.0 / (COARSEN * T))
    adjoints_out[0] = landed_adj[0]
    await_solved(solved, p1)
    states_out[0] = landed[...]

    pl.when(owner)(lambda: sums_spread(b2))

    @pl.when(holds_output)
    def _():
        solved_spread(solved_adj, p2)
        solved_spread(solved, p1)


def emit(*refs):
    for source, target in zip(refs[:3], refs[3:]):
        target[...] = source[...]


def solution(mesh):
    T, X = mesh.shape["tm"], mesh.shape["space"]

    def shards(control, initial, diffusion, reaction, forward_guess, adjoint_guess, observed):
        rows, cols = control.shape
        grid_rows = rows * X
        tiles = (grid_rows // SUB) * (cols // LANES)
        own_tiles = (rows // SUB) * (cols // LANES)
        vmem = pl.BlockSpec(memory_space=pltpu.VMEM)
        f32 = lambda *shape: pltpu.VMEM(shape, jnp.float32)
        dma = lambda *shape: pltpu.SemaphoreType.DMA(shape)
        outs = pl.pallas_call(
            functools.partial(kernel, T, X),
            out_shape=(
                jax.ShapeDtypeStruct(forward_guess.shape, jnp.float32),
                jax.ShapeDtypeStruct(forward_guess.shape, jnp.float32),
                jax.ShapeDtypeStruct(control.shape, jnp.float32),
            ),
            in_specs=[pl.BlockSpec(memory_space=pl.ANY)] * 7,
            out_specs=(vmem,) * 3,
            scratch_shapes=[
                f32(SLOTS, grid_rows, cols),
                f32(rows, cols),
                f32(grid_rows, cols),
                f32(grid_rows, cols),
                f32(COARSEN - 1, grid_rows, cols),
                f32(grid_rows, cols),
                f32(SUMS, grid_rows, cols),
                f32(T, SUB, LANES),
                f32(T, SUB, LANES),
                f32(T, SUB, LANES),
                f32(T, SUB, LANES),
                f32(T, 2, SUB, LANES),
                f32(SUMS, SUB, LANES),
                f32(rows, cols),
                f32(2, rows, cols),
                dma(8),
                pltpu.SemaphoreType.REGULAR(((T - 2).bit_length(),)),
                dma(SLOTS, X), dma(SLOTS, X),
                *[dma(2)] * 8,
            ],
            compiler_params=pltpu.CompilerParams(collective_id=0, has_side_effects=True),
        )(control, initial, diffusion, reaction, forward_guess, adjoint_guess, observed)
        return pl.pallas_call(
            emit,
            out_shape=tuple(jax.ShapeDtypeStruct(out.shape, out.dtype) for out in outs),
            in_specs=[vmem] * 3,
            out_specs=(vmem,) * 3,
        )(*outs)

    return jax.shard_map(
        shards,
        mesh=mesh,
        in_specs=(
            P("space", None),
            P("space", None),
            P("space", None),
            P("space", None),
            P("tm", "space", None),
            P("tm", "space", None),
            P("tm", "space", None),
        ),
        out_specs=(P("tm", "space", None), P("tm", "space", None), P("space", None)),
        check_vma=False,
    )
```
